32 devices in a mesh: rep: 4 (over x, core), dp: 4 (over z), tp: 2 (over y).
Axes of the slice: x: 2, y: 2, z: 4, core: 2. Of those that a mesh axis runs over, the one named last changes fastest.
Arguments:
- hidden: bfloat16 [4, 512, 14336], P('rep', None, 'tp'), may hold values from -6 to 6
- down_weight: bfloat16 [14336, 8192], P('tp', 'dp'), may hold values from -0.046875 to 0.046875
- out_grad: bfloat16 [4, 512, 8192], P('rep', 'tp', 'dp'), may hold values from -6 to 6
- pseudo_grad: bfloat16 [4, 14336, 8192], P('rep', 'tp', 'dp'), may hold values from -6 to 6
- momentum: float32 [14336, 8192], P(('tp', 'rep'), 'dp'), may hold values from -6 to 6
Outputs:
- layer_out: bfloat16 [4, 512, 8192], P('rep', 'tp', 'dp')
- hidden_grad: bfloat16 [4, 512, 14336], P('rep', 'dp', 'tp')
- new_momentum: float32 [14336, 8192], P(('tp', 'rep'), 'dp')
- outer_step: bfloat16 [14336, 8192], P('tp', 'dp')
The draws below stay inside these ranges and needn't reach their ends.
All inputs are finite; a program needn't handle non-finite values.
Results may differ from the reference program's by a relative error of at most 0.017.
Values may be sent and summed in bfloat16 or wider, within the bound.
No kernel may reach another device: no remote copies, remote signals or barrier semaphores. Data moves between devices by JAX's collectives and lax.ppermute only.
A program may use at most 256 MiB of HBM per device.

```python
import jax
import jax.numpy as jnp
from jax import lax

D = 8192
FF = 14336
TOKENS = 512
N_REP = 4
N_DP = 4
N_TP = 2


def block_scale(key, extent, cuts, low, largest):
    gain = 1.0
    for axis_at, parts in cuts:
        heights = jax.random.uniform(jax.random.fold_in(jax.random.fold_in(key, 6), axis_at), (parts,), jnp.float32, low / len(cuts), largest / len(cuts))
        gain = gain * jnp.repeat(jnp.exp(heights), extent[axis_at] // parts).reshape((-1,) + (1,) * (len(extent) - 1 - axis_at))
    return gain


def bell_draw(rng, dims, spread, reach, cuts=(), kind=jnp.bfloat16):
    level = block_scale(rng, dims, cuts, -0.22, 0.18) if cuts else 1.0
    array = jax.random.normal(rng, dims, jnp.float32) * spread * level
    return jnp.minimum(jnp.maximum(array, -reach), reach).astype(kind)


def setup_inputs(seed: int = 0) -> dict:
    key_list = jax.random.split(jax.random.key(seed), 6)
    return {
        "hidden": bell_draw(key_list[0], (N_REP, TOKENS, FF), 1.0, 6.0, ((0, 4), (2, 2))),
        "down_weight": bell_draw(key_list[1], (FF, D), FF ** -0.5, 0.046875, ((0, 2), (1, 4))),
        "out_grad": bell_draw(key_list[2], (N_REP, TOKENS, D), 1.0, 6.0, ((0, 4), (1, 2), (2, 4))),
        "pseudo_grad": bell_draw(key_list[3], (N_REP, FF, D), 1.0, 6.0, ((0, 4), (1, 2), (2, 4))),
        "momentum": bell_draw(key_list[4], (FF, D), 1.0, 6.0, ((0, 8), (1, 4)), jnp.float32),
    }


outer_rate = 0.7
momentum_rate = 0.9


def reference(hidden, down_weight, out_grad, pseudo_grad, momentum):
    hidden_width = FF // N_TP
    model_width = D // N_DP
    weight_tp = down_weight.reshape(N_TP, hidden_width, D)
    weight_dp = jnp.transpose(down_weight.reshape(FF, N_DP, model_width), (1, 0, 2))

    def forward_block(paired):
        return jnp.dot(paired[0], paired[1], preferred_element_type=jnp.float32).astype(jnp.bfloat16)

    def backward_block(paired):
        product = lax.dot_general(paired[0], paired[1], (((1,), (1,)), ((), ())), preferred_element_type=jnp.float32)
        return product.astype(jnp.bfloat16)

    def one_replica(paired):
        token_rows = paired[0]
        grad_rows = paired[1]
        rows_tp = jnp.transpose(token_rows.reshape(TOKENS, N_TP, hidden_width), (1, 0, 2))
        partial_out = lax.map(forward_block, (rows_tp, weight_tp))
        layer = jnp.sum(partial_out.astype(jnp.float32), axis=0).astype(jnp.bfloat16)
        grads_dp = jnp.transpose(grad_rows.reshape(TOKENS, N_DP, model_width), (1, 0, 2))
        partial_back = lax.map(backward_block, (grads_dp, weight_dp))
        back = jnp.sum(partial_back.astype(jnp.float32), axis=0).astype(jnp.bfloat16)
        return layer, back

    layer_out, hidden_grad = lax.map(one_replica, (hidden, out_grad))

    def accumulate(index, running_sum):
        return running_sum + pseudo_grad[index].astype(jnp.float32)

    totals = lax.fori_loop(0, N_REP, accumulate, jnp.zeros((FF, D), jnp.float32))
    average = totals / N_REP
    new_momentum = momentum_rate * momentum + average
    outer_step = (outer_rate * (average + momentum_rate * new_momentum)).astype(jnp.bfloat16)
    return layer_out, hidden_grad, new_momentum, outer_step
```

```python
import jax
import jax.numpy as jnp
from jax import lax
from jax.sharding import PartitionSpec as P


outer_rate = 0.7
momentum_rate = 0.9
piece_units = (1, 3, 5, 4, 1)


def piece_sizes(rows, tile=16):
    if rows % (sum(piece_units) * tile) == 0:
        return [rows // sum(piece_units) * u for u in piece_units]
    return [rows]


def after(index, value):
    return lax.optimization_barrier((index, value))[0]


def outer_update(pseudo, momentum):
    replicas = lax.axis_size("rep")
    lanes = 2 if replicas % 2 == 0 else 1
    groups = replicas // lanes
    me = lax.axis_index("rep")
    lane, group = me % lanes, me // lanes
    mate_perm = [(r, r ^ 1) for r in range(replicas)]
    rows, width = momentum.shape
    sizes = piece_sizes(rows)
    starts = [sum(sizes[:j]) for j in range(len(sizes))]
    pieces = range(len(sizes))
    shifts = range(1, groups)

    def to_mate(value):
        return lax.ppermute(value, "rep", mate_perm)

    def to_group(value, shift):
        perm = [(r, (r // lanes + shift) % groups * lanes + r % lanes) for r in range(replicas)]
        return lax.ppermute(value, "rep", perm)

    def block_of(shift, mate):
        owner = (group + shift) % groups * lanes + (lanes - 1 - lane if mate else lane)
        return owner * rows

    def chip_sum(shift, j, last):
        mine, theirs = block_of(shift, False) + starts[j], block_of(shift, True) + starts[j]
        if last is not None:
            mine, theirs = after((mine, theirs), last)
        total = lax.dynamic_slice(pseudo, (mine, 0), (sizes[j], width)).astype(jnp.float32)
        if lanes == 2:
            other = to_mate(lax.dynamic_slice(pseudo, (theirs, 0), (sizes[j], width)))
            total = total + other.astype(jnp.float32)
        return total

    last = None
    incoming = [[] for _ in pieces]
    for j in pieces:
        for s in shifts:
            value = chip_sum(s, j, last).astype(jnp.bfloat16)
            incoming[j].append(to_group(value, s))
            last = value
    sent = last
    new_momentum = jnp.zeros_like(momentum)
    outer_step = jnp.zeros_like(pseudo)
    own_mine, own_theirs = block_of(0, False), block_of(0, True)
    if sent is not None:
        own_mine, own_theirs = after((own_mine, own_theirs), sent)
    own = None
    if lanes == 2:
        own = to_mate(lax.dynamic_slice(pseudo, (own_theirs, 0), (rows, width)))
    returned = []
    for j in pieces:
        total = lax.dynamic_slice(pseudo, (own_mine + starts[j], 0), (sizes[j], width))
        total = total.astype(jnp.float32)
        if own is not None:
            total = total + lax.slice_in_dim(own, starts[j], starts[j] + sizes[j]).astype(
                jnp.float32
            )
        for piece in incoming[j]:
            total = total + piece.astype(jnp.float32)
        average = total / replicas
        old = lax.slice_in_dim(momentum, starts[j], starts[j] + sizes[j], axis=0)
        fresh = momentum_rate * old + average
        share = (outer_rate * (average + momentum_rate * fresh)).astype(jnp.bfloat16)
        new_momentum = lax.dynamic_update_slice(new_momentum, fresh, (starts[j], 0))
        returned.append([(s, to_group(share, s)) for s in shifts])
        outer_step = lax.dynamic_update_slice(
            outer_step, share, (block_of(0, False) + starts[j], 0)
        )
        if lanes == 2:
            outer_step = lax.dynamic_update_slice(
                outer_step, to_mate(share), (block_of(0, True) + starts[j], 0)
            )
    for j in pieces:
        for s, mine in returned[j]:
            outer_step = lax.dynamic_update_slice(
                outer_step, mine, (block_of(-s, False) + starts[j], 0)
            )
            if lanes == 2:
                outer_step = lax.dynamic_update_slice(
                    outer_step, to_mate(mine), (block_of(-s, True) + starts[j], 0)
                )
    return new_momentum, outer_step, sent


def per_device(hidden, down_weight, out_grad, pseudo_grad, momentum):
    new_momentum, outer_step, _ = outer_update(pseudo_grad[0], momentum)
    partial_out = jnp.dot(hidden[0], down_weight, preferred_element_type=jnp.float32)
    layer_out = lax.psum_scatter(
        partial_out.astype(jnp.bfloat16), "tp", scatter_dimension=0, tiled=True
    )
    all_grads = lax.all_gather(out_grad[0], "tp", axis=0, tiled=True)
    partial_back = lax.dot_general(
        all_grads, down_weight, (((1,), (1,)), ((), ())), preferred_element_type=jnp.float32
    )
    hidden_grad = lax.psum_scatter(
        partial_back.astype(jnp.bfloat16), "dp", scatter_dimension=0, tiled=True
    )
    return (layer_out[None], hidden_grad[None], new_momentum, outer_step)


def solution(mesh):
    return jax.shard_map(
        per_device,
        mesh=mesh,
        in_specs=(
            P("rep", None, "tp"),
            P("tp", "dp"),
            P("rep", "tp", "dp"),
            P("rep", "tp", "dp"),
            P(("tp", "rep"), "dp"),
        ),
        out_specs=(
            P("rep", "tp", "dp"),
            P("rep", "dp", "tp"),
            P(("tp", "rep"), "dp"),
            P("tp", "dp"),
        ),
        check_vma=False,
    )
```
